32 devices in a mesh: samples: 4 (over y, x), features: 4 (over z), rhs: 2 (over core).
Axes of the slice: x: 2, y: 2, z: 4, core: 2. Of those that a mesh axis runs over, the one named last changes fastest.
Arguments:
- design: bfloat16 [32768, 32768], P(('samples', 'rhs'), 'features'), may hold values from -0.03125 to 0.03125
- right_side: float32 [32768, 64], P('features', 'rhs'), may hold values from -6 to 6
- factor: bfloat16 [32768, 768], P('features', 'rhs'), may hold values from -0.03125 to 0.03125
- nystrom_values: float32 [768], replicated, may hold values from 0.5 to 3
Outputs:
- solution: float32 [32768, 64], P('features', 'rhs')
- residual: float32 [32768, 64], P('features', 'rhs')
The draws below stay inside these ranges and needn't reach their ends.
All inputs are finite; a program needn't handle non-finite values.
Results may differ from the reference program's by a relative error of at most 0.0181.
Values may be sent and summed in bfloat16 or wider, within the bound.
A program may use at most 192 MiB of HBM per device.

```python
import math
import jax
import jax.numpy as jnp
from jax import lax

F = 32768
K = 64
R = 768
ITERS = 3
NS = 32768


def block_levels(key, shape, cuts, low, top_value):
    level, own = 1.0, jax.random.fold_in(key, 6)
    for dim, shards_of in cuts:
        steps = jnp.exp(jax.random.uniform(jax.random.fold_in(own, dim), (shards_of,), jnp.float32, low / len(cuts), top_value / len(cuts)))
        level = level * jnp.repeat(steps, shape[dim] // shards_of).reshape([-1 if axis == dim else 1 for axis in range(len(shape))])
    return level


def scatter_about(rng, extent, deviation, most, pieces=(), held_as=jnp.bfloat16):
    factor_of = block_levels(rng, extent, pieces, -0.22, 0.18) if pieces else 1.0
    array = jax.random.normal(rng, extent, jnp.float32) * deviation * factor_of
    return jnp.minimum(jnp.maximum(array, -most), most).astype(held_as)


def setup_inputs(seed: int = 0) -> dict:
    splits = jax.random.split(jax.random.key(seed), 5)
    design = scatter_about(splits[0], (NS, F), NS ** -0.5, 0.03125, ((0, 8), (1, 4)))
    right_side = scatter_about(splits[1], (F, K), 1.0, 6.0, ((0, 4), (1, 2)), jnp.float32)
    factor = scatter_about(splits[2], (F, R), F ** -0.5, 0.03125, ((0, 4), (1, 2)))
    nystrom_values = jnp.clip(jnp.exp(jax.random.uniform(splits[3], (R,), jnp.float32, math.log(0.5), math.log(3.0))), 0.5, 3.0)
    return {"design": design, "right_side": right_side, "factor": factor, "nystrom_values": nystrom_values}


ridge_weight = 1.0

def inner_prod(left, right):
    return lax.dot_general(left.astype(jnp.float32), right.astype(jnp.float32), (((0,), (0,)), ((), ())), precision=lax.Precision.HIGHEST, preferred_element_type=jnp.float32)

def apply_operator(design, direction):
    narrow = direction.astype(jnp.bfloat16)
    images = jnp.dot(design.astype(jnp.float32), narrow.astype(jnp.float32), preferred_element_type=jnp.float32).astype(jnp.bfloat16)
    summed = lax.dot_general(design.astype(jnp.float32), images.astype(jnp.float32), (((0,), (0,)), ((), ())), preferred_element_type=jnp.float32)
    return summed + ridge_weight * direction

def reference(design, right_side, factor, nystrom_values):
    shrink = (1.0 + jnp.min(nystrom_values)) / (1.0 + nystrom_values) - 1.0
    factor_wide = factor.astype(jnp.float32)

    def precondition(values):
        projected = inner_prod(factor_wide, values)
        return values + jnp.dot(factor_wide, shrink[:, None] * projected, precision=lax.Precision.HIGHEST)
    solution = jnp.zeros_like(right_side)
    residual = right_side
    direction = precondition(residual)
    for iteration in range(ITERS):
        applied = apply_operator(design, direction)
        gram_block = inner_prod(direction, applied)
        gram_block = 0.5 * (gram_block + gram_block.T)
        chol_lower = jnp.linalg.cholesky(gram_block)
        unit_dir = jax.scipy.linalg.solve_triangular(chol_lower, direction.T, lower=True).T
        unit_img = jax.scipy.linalg.solve_triangular(chol_lower, applied.T, lower=True).T
        step_coef = jax.scipy.linalg.solve_triangular(chol_lower, inner_prod(direction, residual), lower=True)
        solution = solution + jnp.dot(unit_dir, step_coef, precision=lax.Precision.HIGHEST)
        residual = residual - jnp.dot(unit_img, step_coef, precision=lax.Precision.HIGHEST)
        if iteration + 1 < ITERS:
            scaled = precondition(residual)
            next_coef = -inner_prod(unit_img, scaled)
            direction = scaled + jnp.dot(unit_dir, next_coef, precision=lax.Precision.HIGHEST)
    return (solution, residual)
```

```python
import functools

import jax
import jax.numpy as jnp
from jax import lax
from jax.experimental import pallas as pl
from jax.experimental.pallas import tpu as pltpu
from jax.sharding import PartitionSpec as P

ITERS = 3
MESH = pl.DeviceIdType.MESH
RIDGE = 1.0
EARLY = 2
LATE = 2


def dot_t(left, right):
    return lax.dot_general(
        left,
        right,
        (((1,), (1,)), ((), ())),
        precision=lax.Precision.HIGHEST,
        preferred_element_type=jnp.float32,
    )


def dot_h(left, right):
    return jnp.dot(
        left, right, precision=lax.Precision.HIGHEST, preferred_element_type=jnp.float32
    )


def feature_group(n_rhs):
    me = lax.axis_index("samples") * n_rhs + lax.axis_index("rhs")

    def place(index):
        return {"samples": lax.div(index, n_rhs), "rhs": lax.rem(index, n_rhs)}

    return me, place


def sample_group():
    return lax.axis_index("features"), lambda index: {"features": index}


def others(n, me, body):
    for step in range(1, n):
        body(lax.rem(me + step, n))


def greet(groups):
    barrier = pltpu.get_barrier_semaphore()
    total = 0
    for n, me, place in groups:
        others(
            n,
            me,
            lambda peer: pl.semaphore_signal(
                barrier, inc=1, device_id=place(peer), device_id_type=MESH
            ),
        )
        total += n - 1
    pl.semaphore_wait(barrier, total)


def columns(index, width):
    return pl.ds(pl.multiple_of(index * width, 128), width)


def exchange(n, me, place, source, target, send_sem, recv_sem):
    def copy(step):
        peer = lax.rem(me + step, n)
        return pltpu.make_async_remote_copy(
            src_ref=source(peer),
            dst_ref=target(me),
            send_sem=send_sem.at[step],
            recv_sem=recv_sem.at[step],
            device_id=place(peer),
            device_id_type=MESH,
        )

    copies = [copy(step) for step in range(1, n)]
    for each in copies:
        each.start()
    for each in copies:
        each.wait_recv()
    return copies


def finish(copies):
    for each in copies:
        each.wait_send()


def total_of(own, held, n, me):
    total = own.astype(jnp.float32)
    for step in range(1, n):
        total = total + held[lax.rem(me + step, n)].astype(jnp.float32)
    return total


def other_index(me, step, n):
    if n & (n - 1):
        return None
    bit, total = 1, 0
    while bit < n:
        total = total + ((me // bit + step // bit) % 2) * bit
        bit *= 2
    return total


def operator_kernel(
    n_samp, n_rhs, n_feat, early, late,
    x_ref, design, out_ref,
    slots, narrow, acc, part, up, cross, images, give, side, side_in, chip, chip_in, own,
    load_sem, piece_send, piece_recv, twin_send, twin_recv,
    up_send, up_recv, cross_recv, down_send, down_recv,
    side_send, side_recv, chip_send, chip_recv,
):
    samp, core = lax.axis_index("samples"), lax.axis_index("rhs")
    feat = lax.axis_index("features")
    n = n_samp * n_rhs
    count, width, chunk = part.shape
    held = slots.shape[0]
    piece = x_ref.shape[1]
    half = n_feat // 2
    low = feat < half
    inner = jnp.logical_or(feat == half - 1, feat == half)
    outer = jnp.logical_not(inner)
    first_end, last_end = feat == 0, feat == n_feat - 1
    is_end = jnp.logical_or(first_end, last_end)
    has_prev = jnp.logical_not(is_end)
    following = jnp.where(low, feat + 1, feat - 1)
    before = jnp.where(low, feat - 1, feat + 1)

    def chip_of(step):
        return other_index(samp, step, n_samp)

    def core_of(step):
        return other_index(core, step, n_rhs)

    def cols(chip_index, core_index):
        return columns(chip_index * n_rhs + core_index, piece)

    def load(c):
        return pltpu.make_async_copy(
            design.at[pl.ds(pl.multiple_of(c * chunk, chunk), chunk), :],
            slots.at[lax.rem(c, held)],
            load_sem.at[lax.rem(c, held)],
        )

    def remote(src, dst, send, recv, where):
        return pltpu.make_async_remote_copy(
            src_ref=src, dst_ref=dst, send_sem=send, recv_sem=recv,
            device_id=where, device_id_type=MESH,
        )

    def loop(low_bound, high_bound, body):
        def step(i, carry):
            body(i)
            return carry

        lax.fori_loop(low_bound, high_bound, step, 0)

    loop(0, held, lambda c: load(c).start())

    barrier = pltpu.get_barrier_semaphore()

    def signal(where):
        pl.semaphore_signal(barrier, inc=1, device_id=where, device_id_type=MESH)

    for step in range(1, n_samp):
        signal({"samples": chip_of(step)})
    for step in range(1, n_rhs):
        signal({"rhs": core_of(step)})

    @pl.when(jnp.logical_not(first_end))
    def _():
        signal({"features": feat - 1})

    @pl.when(jnp.logical_not(last_end))
    def _():
        signal({"features": feat + 1})

    greeted = n_samp - 1 + n_rhs - 1
    pl.semaphore_wait(
        barrier, jnp.where(is_end, greeted + 1, greeted + 2) if n_feat > 1 else greeted
    )

    def piece_copy(step):
        return remote(
            x_ref, narrow.at[:, cols(samp, core)], piece_send.at[step], piece_recv.at[step],
            {"samples": chip_of(step)},
        )

    def twin_copy(step, other):
        held_piece = narrow.at[:, cols(chip_of(step), core)]
        return remote(
            held_piece, held_piece, twin_send.at[step, other], twin_recv.at[step, other],
            {"rhs": core_of(other)},
        )

    for step in range(1, n_samp):
        piece_copy(step).start()
    narrow[:, cols(samp, core)] = x_ref[...]

    def first_terms(place_cols, fresh):
        for c in range(early):
            term = lax.dot_general(
                narrow[:, place_cols], slots[c, :, place_cols],
                (((1,), (1,)), ((), ())), preferred_element_type=jnp.float32,
            )
            part[c] = part[c] + term

    for c in range(early):
        part[c] = jnp.zeros((width, chunk), jnp.float32)
    acc[...] = jnp.zeros_like(acc)
    for c in range(early):
        load(c).wait()

    def arrive(step):
        @pl.when(step > 0)
        def _():
            piece_copy(step).wait_recv()

        for other in range(1, n_rhs):
            twin_copy(step, other).start()

        def by_core(other):
            @pl.when(other > 0)
            def _():
                twin_copy(step, other).wait_recv()

            first_terms(cols(chip_of(step), core_of(other)), False)

        loop(0, n_rhs, by_core)

    loop(0, n_samp, arrive)

    def up_copy(c):
        return remote(
            give.at[c], up.at[c], up_send.at[c], up_recv.at[c], {"features": following}
        )

    def cross_copy(c):
        return remote(
            give.at[c], cross.at[c], up_send.at[c], cross_recv.at[c], {"features": following}
        )

    def down_copy(c):
        return remote(
            images.at[c], images.at[c], down_send.at[c], down_recv.at[c], {"features": before}
        )

    def pass_up(c):
        @pl.when(inner)
        def _():
            cross_copy(c).start()

        @pl.when(outer)
        def _():
            up_copy(c).start()

    def up_first(c):
        @pl.when(is_end)
        def _():
            give[c] = part[c].astype(give.dtype)
            pass_up(c)

    def up_step(c):
        @pl.when(has_prev)
        def _():
            up_copy(c).wait_recv()
            total = part[c] + up[c].astype(jnp.float32)
            part[c] = total
            give[c] = total.astype(give.dtype)
            pass_up(c)

    def cross_step(c):
        @pl.when(inner)
        def _():
            cross_copy(c).wait_recv()
            images[c] = (part[c] + cross[c].astype(jnp.float32)).astype(images.dtype)

            @pl.when(has_prev)
            def _():
                down_copy(c).start()

    def ready(c):
        @pl.when(outer)
        def _():
            down_copy(c).wait_recv()

            @pl.when(has_prev)
            def _():
                down_copy(c).start()

    def image_step(c):
        load(c).wait()
        part[c] = lax.dot_general(
            narrow[...], slots[lax.rem(c, held)],
            (((1,), (1,)), ((), ())), preferred_element_type=jnp.float32,
        )
        up_first(c)
        loop(jnp.where(c == early, 0, c - 1), c, up_step)
        loop(jnp.where(c == early + 1, 0, jnp.where(c == early, 0, c - 2)),
             jnp.where(c == early, 0, c - 1), cross_step)

    def feature_step(c):
        ready(c)
        acc[...] = acc[...] + jnp.dot(
            images[c], slots[lax.rem(c, held)], preferred_element_type=jnp.float32
        )

        @pl.when(c + held < count)
        def _():
            load(c + held).start()

    for c in range(early):
        up_first(c)

    spare = count - held
    middle = spare + max((held - late) // 2 - 1, 0)

    def both_steps(turn):
        loop(jnp.where(turn == 0, early, held), jnp.where(turn == 0, held, count), image_step)

        def step(c):
            feature_step(c)

            @pl.when(jnp.logical_and(turn == 1, c == middle))
            def _():
                up_step(count - 1)
                cross_step(count - 2)

        loop(jnp.where(turn == 0, 0, spare), jnp.where(turn == 0, spare, count - late), step)

    loop(0, 2, both_steps)
    cross_step(count - 1)
    for c in range(count - late, count):
        ready(c)

    def piece_total(place_cols):
        total = acc[:, place_cols]
        for c in range(count - late, count):
            total = total + jnp.dot(
                images[c], slots[c % held, :, place_cols], preferred_element_type=jnp.float32
            )
        return total

    def side_copy(step, other):
        return remote(
            side.at[step, other], side_in.at[step, other],
            side_send.at[step, other], side_recv.at[step, other], {"rhs": core_of(other)},
        )

    def chip_copy(step):
        return remote(
            chip.at[step], chip_in.at[step], chip_send.at[step], chip_recv.at[step],
            {"samples": chip_of(step)},
        )

    def chip_total(step):
        total = own[...]
        for other in range(1, n_rhs):
            side_copy(step, other).wait_recv()
            total = total + side_in[step, other].astype(jnp.float32)
        return total

    def leave(i):
        step = n_samp - 1 - i

        def by_core(j):
            other = n_rhs - 1 - j
            total = piece_total(cols(chip_of(step), core_of(other)))

            @pl.when(other > 0)
            def _():
                side[step, other] = total.astype(side.dtype)
                side_copy(step, other).start()

            @pl.when(jnp.logical_and(other == min(1, n_rhs - 1), step < n_samp - 1))
            def _():
                chip[step + 1] = chip_total(step + 1).astype(chip.dtype)
                chip_copy(step + 1).start()

            @pl.when(other == 0)
            def _():
                own[...] = total

        loop(0, n_rhs, by_core)

    loop(0, n_samp, leave)
    out = chip_total(0)
    for step in range(n_samp - 1, 0, -1):
        chip_copy(step).wait_recv()
        out = out + chip_in[step].astype(jnp.float32)
    out_ref[...] = out

    for step in range(1, n_samp):
        piece_copy(step).wait_send()
        chip_copy(step).wait_send()

    def end_core(step):
        for other in range(1, n_rhs):
            twin_copy(step, other).wait_send()
            side_copy(step, other).wait_send()

    loop(0, n_samp, end_core)

    def end_chunk(c):
        up_copy(c).wait_send()

        @pl.when(has_prev)
        def _():
            down_copy(c).wait_send()

    loop(0, count, end_chunk)


def apply_operator(n_samp, n_rhs, n_feat, x, design):
    width, piece = x.shape
    rows, feats = design.shape
    chunk = min(512, rows // 4)
    count = rows // chunk
    held = min(count, (48 << 20) // (chunk * feats * 2))
    wide = (width, piece)
    blocks = (count, width, chunk)
    vmem, dma = pltpu.VMEM, pltpu.SemaphoreType.DMA
    bf16, f32 = jnp.bfloat16, jnp.float32
    return pl.pallas_call(
        functools.partial(operator_kernel, n_samp, n_rhs, n_feat, EARLY, LATE),
        name="operator",
        out_shape=jax.ShapeDtypeStruct(wide, f32),
        in_specs=[pl.BlockSpec(memory_space=vmem), pl.BlockSpec(memory_space=pl.ANY)],
        out_specs=pl.BlockSpec(memory_space=vmem),
        scratch_shapes=[
            vmem((held, chunk, feats), bf16), vmem((width, feats), bf16), vmem((width, feats), f32),
            vmem(blocks, f32), vmem(blocks, bf16), vmem(blocks, bf16), vmem(blocks, bf16),
            vmem(blocks, bf16),
            vmem((n_samp, n_rhs) + wide, bf16), vmem((n_samp, n_rhs) + wide, bf16),
            vmem((n_samp,) + wide, bf16), vmem((n_samp,) + wide, bf16), vmem(wide, f32),
            dma((held,)), dma((n_samp,)), dma((n_samp,)), dma((n_samp, n_rhs)), dma((n_samp, n_rhs)),
            dma((count,)), dma((count,)), dma((count,)), dma((count,)), dma((count,)),
            dma((n_samp, n_rhs)), dma((n_samp, n_rhs)), dma((n_samp,)), dma((n_samp,)),
        ],
        compiler_params=pltpu.CompilerParams(
            collective_id=1, has_side_effects=True, vmem_limit_bytes=60 << 20
        ),
    )(x, design)


def gather_kernel(n, n_rhs, split, x_ref, out_ref, send_a, recv_a):
    me, place = feature_group(n_rhs)
    rows, wide = out_ref.shape
    width = wide // n

    def part(peer):
        if split:
            return pl.ds(pl.multiple_of(lax.rem(peer, n_rhs) * rows, 16), rows)
        return pl.ds(0, rows)

    greet([(n, me, place)])
    first = exchange(
        n, me, place,
        lambda peer: x_ref.at[part(peer), :],
        lambda index: out_ref.at[:, columns(index, width)],
        send_a, recv_a,
    )
    out_ref[:, columns(me, width)] = x_ref[part(me), :]
    finish(first)


def totals_kernel(
    n, n_rhs, n_feat, x_ref, out_ref, held, across, mine, sa, ra, sb, rb, sc, rc
):
    me, place = feature_group(n_rhs)
    feat, feat_place = sample_group()
    width = x_ref.shape[1] // n
    greet([(n, me, place), (n_feat, feat, feat_place)])
    first = exchange(
        n, me, place,
        lambda peer: x_ref.at[:, columns(peer, width)],
        lambda index: held.at[index],
        sa, ra,
    )
    mine[...] = total_of(x_ref[:, columns(me, width)], held, n, me)
    second = exchange(
        n_feat, feat, feat_place,
        lambda peer: mine,
        lambda index: across.at[index],
        sb, rb,
    )
    across[feat] = mine[...]
    total = across[0]
    for index in range(1, n_feat):
        total = total + across[index]
    out_ref[:, columns(me, width)] = total
    third = exchange(
        n, me, place,
        lambda peer: out_ref.at[:, columns(me, width)],
        lambda index: out_ref.at[:, columns(index, width)],
        sc, rc,
    )
    finish(first + second + third)


def call(kernel, name, ident, shape, dtype, scratch, sems, *args):
    return pl.pallas_call(
        kernel,
        name=name,
        out_shape=jax.ShapeDtypeStruct(shape, dtype),
        in_specs=[pl.BlockSpec(memory_space=pltpu.VMEM)] * len(args),
        out_specs=pl.BlockSpec(memory_space=pltpu.VMEM),
        scratch_shapes=[pltpu.VMEM(s, d) for s, d in scratch]
        + [pltpu.SemaphoreType.DMA((count,)) for count in sems],
        compiler_params=pltpu.CompilerParams(collective_id=ident, has_side_effects=True),
    )(*args)


def shards(n_samp, n_feat, n_rhs, design, right_side, factor, nystrom_values):
    feat_rows, col_share = right_side.shape
    samples = design.shape[0]
    width = col_share * n_rhs
    rank = nystrom_values.shape[0]
    n = n_samp * n_rhs
    piece = feat_rows // n
    samp, rhs = lax.axis_index("samples"), lax.axis_index("rhs")
    shrink = (1.0 + jnp.min(nystrom_values)) / (1.0 + nystrom_values) - 1.0

    def own_rows(block):
        def rows_for(core):
            return lax.dynamic_slice_in_dim(block, (samp * n_rhs + core) * piece, piece, 0)

        parts = [None] * n_rhs
        moved = [rows_for(rhs)]
        for step in range(1, n_rhs):
            pairs = [(i, (i + step) % n_rhs) for i in range(n_rhs)]
            moved.append(lax.ppermute(rows_for((rhs + step) % n_rhs), "rhs", pairs))
        for core in range(n_rhs):
            best = moved[0]
            for step in range(1, n_rhs):
                best = jnp.where((rhs - step) % n_rhs == core, moved[step], best)
            parts[core] = best
        return jnp.concatenate(parts, axis=1)

    gather_out = lambda x: call(
        functools.partial(gather_kernel, n, n_rhs, True), "output_gather", 4,
        (x.shape[0] // n_rhs, feat_rows), x.dtype, [], [n] * 2, x,
    )

    def totals(x):
        lanes = x.shape[1]
        unit = 128 * n
        padded = -(-lanes // unit) * unit
        x = jnp.pad(x, ((0, 0), (0, padded - lanes)))
        share = (width, padded // n)
        got = call(
            functools.partial(totals_kernel, n, n_rhs, n_feat), "small_totals", 5,
            x.shape, jnp.float32,
            [((n,) + share, jnp.float32), ((n_feat,) + share, jnp.float32), (share, jnp.float32)],
            [n, n, n_feat, n_feat, n, n], x,
        )
        return got[:, :lanes]

    basis = own_rows(factor)
    residual = own_rows(right_side).T

    def parts_of(values):
        upper = values.astype(jnp.bfloat16)
        widened = lax.optimization_barrier(upper).astype(jnp.float32)
        return jnp.concatenate([upper, (values - widened).astype(jnp.bfloat16)], axis=0)

    def factor_inner(values):
        both = jnp.dot(parts_of(values), basis, preferred_element_type=jnp.float32)
        return both[:width] + both[width:]

    def expand(projected):
        both = lax.dot_general(
            parts_of(shrink[None, :] * projected), basis, (((1,), (1,)), ((), ())),
            preferred_element_type=jnp.float32,
        )
        return both[:width] + both[width:]

    projected = totals(factor_inner(residual))
    direction = residual + expand(projected)
    solution = jnp.zeros_like(residual)
    eye = jnp.eye(width, dtype=jnp.float32)
    for iteration in range(ITERS):
        summed_features = apply_operator(
            n_samp, n_rhs, n_feat, direction.astype(jnp.bfloat16), design
        )
        applied = summed_features + RIDGE * direction
        last = iteration + 1 == ITERS
        block = dot_t(
            jnp.concatenate([direction, applied], axis=0),
            jnp.concatenate([applied, residual], axis=0),
        )
        small = [block[:width], block[width:]]
        if not last:
            small.append(factor_inner(applied))
        summed = totals(jnp.concatenate(small, axis=1))
        gram = summed[:, :width]
        cross = summed[:, width : 2 * width]
        gram = 0.5 * (gram + gram.T)
        chol_lower = jnp.linalg.cholesky(gram)
        inverse = jax.scipy.linalg.solve_triangular(chol_lower, eye, lower=True)
        back_t = dot_h(dot_h(inverse, cross).T, inverse)
        solution = solution + dot_h(back_t, direction)
        residual = residual - dot_h(back_t, applied)
        if not last:
            image_image = summed[:, 2 * width : 3 * width]
            image_res = summed[:, 3 * width : 4 * width]
            factor_image = summed[:, 4 * width :]
            projected = projected - dot_h(back_t, factor_image)
            scaled = residual + expand(projected)
            image_new = image_res - dot_t(image_image, back_t)
            image_new = image_new + dot_t(factor_image, shrink[None, :] * projected)
            next_t = dot_h(dot_h(inverse, image_new).T, inverse)
            direction = scaled - dot_h(next_t, direction)
    stacked = []
    for core in range(n_rhs):
        rows = slice(core * col_share, (core + 1) * col_share)
        stacked += [solution[rows], residual[rows]]
    whole = gather_out(jnp.concatenate(stacked, axis=0).astype(jnp.bfloat16))
    whole = whole.astype(jnp.float32)
    return whole[:col_share].T, whole[col_share:].T


def solution(mesh):
    placed = (P(("samples", "rhs"), "features"), P("features", "rhs"), P("features", "rhs"), P())
    sizes = (mesh.shape["samples"], mesh.shape["features"], mesh.shape["rhs"])
    return jax.shard_map(
        functools.partial(shards, *sizes),
        mesh=mesh,
        in_specs=placed,
        out_specs=(P("features", "rhs"), P("features", "rhs")),
        check_vma=False,
    )
```

```python
import functools

import jax
import jax.numpy as jnp
from jax import lax
from jax.experimental import pallas as pl
from jax.experimental.pallas import tpu as pltpu
from jax.sharding import PartitionSpec as P

ITERS = 3
MESH = pl.DeviceIdType.MESH
RIDGE = 1.0
EARLY = 2
LATE = 2
SLOT_BYTES = 40 << 20


def dot_t(left, right):
    return lax.dot_general(
        left,
        right,
        (((1,), (1,)), ((), ())),
        precision=lax.Precision.HIGHEST,
        preferred_element_type=jnp.float32,
    )


def dot_h(left, right):
    return jnp.dot(
        left, right, precision=lax.Precision.HIGHEST, preferred_element_type=jnp.float32
    )


def columns(index, width):
    return pl.ds(pl.multiple_of(index * width, 128), width)


def partner(me, step, n):
    bit, total = 1, 0
    while bit < n:
        total = total + (me // bit + step // bit) % 2 * bit
        bit *= 2
    return total


def loop(start, stop, body):
    def step(i, carry):
        body(i)
        return carry

    lax.fori_loop(start, stop, step, 0)


def parts_of(values):
    upper = values.astype(jnp.bfloat16)
    lower = (values - upper.astype(jnp.float32)).astype(jnp.bfloat16)
    return jnp.concatenate([upper, lower], axis=0)


def in_parts(values, right, contract):
    rows = values.shape[0]
    both = lax.dot_general(
        parts_of(values), right, (((1,), (contract,)), ((), ())),
        preferred_element_type=jnp.float32,
    )
    return both[:rows] + both[rows:]


def inverse_of(gram):
    size = gram.shape[0]
    rows = lax.broadcasted_iota(jnp.int32, (size, 2 * size), 0)
    lanes = lax.broadcasted_iota(jnp.int32, (size, 2 * size), 1)
    unit = (lanes == rows + size).astype(jnp.float32)
    work = jnp.concatenate([gram, jnp.zeros_like(gram)], axis=1) + unit
    for k in range(size):
        pivot = work[k : k + 1, :] / work[k : k + 1, k : k + 1]
        work = jnp.where(rows == k, pivot, work - work[:, k : k + 1] * pivot)
    return work[:, size:]


def solve_kernel(
    n_samp, n_rhs, n_feat,
    right_ref, basis, shrink_ref, design, sol_out, res_out,
    slots, narrow, acc, part, up, cross, images, give, side, side_in, chip, chip_in, own,
    sent, direction, applied, residual, projected, back_ref, sol, rest, rest_in,
    g_send, g_held, g_mine, g_across, g_out, f_send, f_held, f_mine, f_across, f_out,
    load_sem, out_sem, piece_send, piece_recv, twin_send, twin_recv,
    up_send, up_recv, cross_recv, down_send, down_recv,
    side_send, side_recv, chip_send, chip_recv, rest_send, rest_recv,
    g_sems, gz_sems, f_sems, fz_sems,
):
    samp, core = lax.axis_index("samples"), lax.axis_index("rhs")
    feat = lax.axis_index("features")
    n = n_samp * n_rhs
    me = samp * n_rhs + core
    count, width, chunk = part.shape
    held = slots.shape[0]
    spare = count - held
    piece = right_ref.shape[1]
    share = width // n_rhs
    half = n_feat // 2
    low = feat < half
    inner = jnp.logical_or(feat == half - 1, feat == half)
    outer = jnp.logical_not(inner)
    is_end = jnp.logical_or(feat == 0, feat == n_feat - 1)
    has_prev = jnp.logical_not(is_end)
    following = jnp.where(low, feat + 1, feat - 1)
    before = jnp.where(low, feat - 1, feat + 1)
    f32, bf16 = jnp.float32, jnp.bfloat16

    def place(index):
        return {"samples": lax.div(index, n_rhs), "rhs": lax.rem(index, n_rhs)}

    def chip_of(step):
        return partner(samp, step, n_samp)

    def core_of(step):
        return partner(core, step, n_rhs)

    def cols(chip_index, core_index):
        return columns(chip_index * n_rhs + core_index, piece)

    def remote(src, dst, send, recv, where):
        return pltpu.make_async_remote_copy(
            src_ref=src, dst_ref=dst, send_sem=send, recv_sem=recv,
            device_id=where, device_id_type=MESH,
        )

    def load(place_in_all):
        slot = lax.rem(place_in_all, held)
        row = pl.multiple_of(lax.rem(place_in_all, count) * chunk, chunk)
        return pltpu.make_async_copy(
            design.at[pl.ds(row, chunk), :], slots.at[slot], load_sem.at[slot]
        )

    loop(0, held, lambda c: load(c).start())

    barrier = pltpu.get_barrier_semaphore()
    for step in range(1, n):
        pl.semaphore_signal(
            barrier, inc=1, device_id=place(lax.rem(me + step, n)), device_id_type=MESH
        )
    for step in range(1, n_feat):
        pl.semaphore_signal(
            barrier, inc=1, device_id={"features": lax.rem(feat + step, n_feat)},
            device_id_type=MESH,
        )
    pl.semaphore_wait(barrier, n - 1 + n_feat - 1)

    def totals(send, held_in, mine, across, out, sems, z_sems):
        def scatter(step):
            peer = lax.rem(me + step, n)
            return remote(
                send.at[peer], held_in.at[me], sems.at[0, step], sems.at[1, step], place(peer)
            )

        def along(step):
            peer = lax.rem(feat + step, n_feat)
            return remote(
                mine, across.at[feat], z_sems.at[0, step], z_sems.at[1, step], {"features": peer}
            )

        def gather(step):
            peer = lax.rem(me + step, n)
            return remote(
                out.at[me], out.at[me], sems.at[2, step], sems.at[3, step], place(peer)
            )

        def first():
            for step in range(1, n):
                scatter(step).start()

        def second():
            total = send[me].astype(f32)
            for step in range(1, n):
                scatter(step).wait_recv()
            for step in range(1, n):
                total = total + held_in[lax.rem(me + step, n)].astype(f32)
            mine[...] = total.astype(mine.dtype)
            for step in range(1, n_feat):
                along(step).start()
            across[feat] = total.astype(mine.dtype)

        def third():
            for step in range(1, n_feat):
                along(step).wait_recv()
            total = across[0].astype(f32)
            for index in range(1, n_feat):
                total = total + across[index].astype(f32)
            out[me] = total.astype(out.dtype)
            for step in range(1, n):
                gather(step).start()

        def fourth():
            for step in range(1, n):
                gather(step).wait_recv()

        def end():
            for step in range(1, n):
                scatter(step).wait_send()
                gather(step).wait_send()
            for step in range(1, n_feat):
                along(step).wait_send()

        return first, second, third, fourth, end

    g_first, g_second, g_third, g_fourth, g_end = totals(
        g_send, g_held, g_mine, g_across, g_out, g_sems, gz_sems
    )
    f_first, f_second, f_third, f_fourth, f_end = totals(
        f_send, f_held, f_mine, f_across, f_out, f_sems, fz_sems
    )
    f_rows, f_lanes = f_send.shape[1:]
    g_rows = g_send.shape[1]

    def factor_inner(values):
        inner_product = jnp.dot(values, basis[...], preferred_element_type=f32)
        for s in range(n_samp):
            for c in range(n_rhs):
                block = inner_product[s * f_rows : (s + 1) * f_rows, c * f_lanes : (c + 1) * f_lanes]
                f_send[s * n_rhs + c] = block.astype(bf16)

    def factor_total():
        lines = []
        for s in range(n_samp):
            line = [f_out[s * n_rhs + c].astype(f32) for c in range(n_rhs)]
            lines.append(jnp.concatenate(line, axis=1))
        return jnp.concatenate(lines, axis=0)

    def piece_copy(step, side_of):
        return remote(
            sent, narrow.at[side_of, :, cols(samp, core)], piece_send.at[step],
            piece_recv.at[step], {"samples": chip_of(step)},
        )

    def twin_copy(step, other, side_of):
        block = narrow.at[side_of, :, cols(chip_of(step), core)]
        return remote(
            block, block, twin_send.at[step, other], twin_recv.at[step, other],
            {"rhs": core_of(other)},
        )

    def give_out(values, side_of):
        sent[...] = values.astype(bf16)
        for step in range(1, n_samp):
            piece_copy(step, side_of).start()
        narrow[side_of, :, cols(samp, core)] = values.astype(bf16)

    def take_in(side_of, use):
        def arrive(step):
            @pl.when(step > 0)
            def _():
                piece_copy(step, side_of).wait_recv()

            for other in range(1, n_rhs):
                twin_copy(step, other, side_of).start()

            def by_core(other):
                @pl.when(other > 0)
                def _():
                    twin_copy(step, other, side_of).wait_recv()

                if use is not None:
                    use(cols(chip_of(step), core_of(other)))

            loop(0, n_rhs, by_core)

        loop(0, n_samp, arrive)

    def end_pieces(side_of):
        for step in range(1, n_samp):
            piece_copy(step, side_of).wait_send()
        for step in range(n_samp):
            for other in range(1, n_rhs):
                twin_copy(step, other, side_of).wait_send()

    def up_copy(c):
        return remote(
            give.at[c], up.at[c], up_send.at[c], up_recv.at[c], {"features": following}
        )

    def cross_copy(c):
        return remote(
            give.at[c], cross.at[c], up_send.at[c], cross_recv.at[c], {"features": following}
        )

    def down_copy(c):
        return remote(
            images.at[c], images.at[c], down_send.at[c], down_recv.at[c], {"features": before}
        )

    def pass_up(c):
        @pl.when(inner)
        def _():
            cross_copy(c).start()

        @pl.when(outer)
        def _():
            up_copy(c).start()

    def up_first(c):
        @pl.when(is_end)
        def _():
            give[c] = part[c].astype(bf16)
            pass_up(c)

    def up_step(c):
        @pl.when(has_prev)
        def _():
            up_copy(c).wait_recv()
            total = part[c] + up[c].astype(f32)
            part[c] = total
            give[c] = total.astype(bf16)
            pass_up(c)

    def cross_step(c):
        @pl.when(inner)
        def _():
            cross_copy(c).wait_recv()
            images[c] = (part[c] + cross[c].astype(f32)).astype(bf16)

            @pl.when(has_prev)
            def _():
                down_copy(c).start()

    def ready(c):
        @pl.when(outer)
        def _():
            down_copy(c).wait_recv()

            @pl.when(has_prev)
            def _():
                down_copy(c).start()

    def side_copy(step, other):
        return remote(
            side.at[step, other - 1], side_in.at[step, other - 1],
            side_send.at[step, other], side_recv.at[step, other], {"rhs": core_of(other)},
        )

    def chip_copy(step):
        return remote(
            chip.at[step], chip_in.at[step], chip_send.at[step], chip_recv.at[step],
            {"samples": chip_of(step)},
        )

    def chip_total(step):
        total = own[...]
        for other in range(1, n_rhs):
            side_copy(step, other).wait_recv()
            total = total + side_in[step, other - 1].astype(f32)
        return total

    def operate(turn, side_of):
        base = turn * spare

        def slot_of(c):
            return lax.rem(base + c, held)

        acc[...] = jnp.zeros_like(acc)
        for c in range(EARLY):
            part[c] = jnp.zeros((width, chunk), f32)

        @pl.when(turn == 0)
        def _():
            for c in range(EARLY):
                load(c).wait()

        def first_terms(place_cols):
            for c in range(EARLY):
                part[c] = part[c] + lax.dot_general(
                    narrow[side_of, :, place_cols], slots[slot_of(c), :, place_cols],
                    (((1,), (1,)), ((), ())), preferred_element_type=f32,
                )

        take_in(side_of, first_terms)

        def rest_copy(step):
            peer = lax.rem(me + step, n)
            row = pl.multiple_of(lax.rem(peer, n_rhs) * share, 16)
            return remote(
                rest.at[pl.ds(row, share), :], rest_in.at[:, columns(me, piece)],
                rest_send.at[step], rest_recv.at[step], place(peer),
            )

        @pl.when(turn == ITERS - 1)
        def _():
            rest[...] = residual[...].astype(bf16)
            for step in range(1, n):
                rest_copy(step).start()
            rest_in[:, columns(me, piece)] = rest[pl.ds(pl.multiple_of(core * share, 16), share), :]

        for c in range(EARLY):
            up_first(c)

        def image_step(c):
            @pl.when(jnp.logical_or(turn == 0, c >= held))
            def _():
                load(base + c).wait()

            part[c] = lax.dot_general(
                narrow[side_of], slots[slot_of(c)],
                (((1,), (1,)), ((), ())), preferred_element_type=f32,
            )
            up_first(c)
            loop(jnp.where(c == EARLY, 0, c - 1), c, up_step)
            loop(
                jnp.where(c <= EARLY + 1, 0, c - 2), jnp.where(c == EARLY, 0, c - 1), cross_step
            )

        def feature_step(c):
            ready(c)
            acc[...] = acc[...] + jnp.dot(
                images[c], slots[slot_of(c)], preferred_element_type=f32
            )

            @pl.when(c + held < count)
            def _():
                load(base + c + held).start()

        middle = spare + max((held - LATE) // 2 - 1, 0)

        def both_steps(part_of):
            loop(
                jnp.where(part_of == 0, EARLY, held), jnp.where(part_of == 0, held, count),
                image_step,
            )

            def step(c):
                feature_step(c)

                @pl.when(jnp.logical_and(part_of == 1, c == middle))
                def _():
                    up_step(count - 1)
                    cross_step(count - 2)

            loop(
                jnp.where(part_of == 0, 0, spare), jnp.where(part_of == 0, spare, count - LATE),
                step,
            )

        loop(0, 2, both_steps)
        cross_step(count - 1)
        for c in range(count - LATE, count):
            ready(c)

        def piece_total(place_cols):
            total = acc[:, place_cols]
            for c in range(count - LATE, count):
                total = total + jnp.dot(
                    images[c], slots[slot_of(c), :, place_cols], preferred_element_type=f32
                )
            return total

        def leave(i):
            step = n_samp - 1 - i

            def by_core(j):
                other = n_rhs - 1 - j
                total = piece_total(cols(chip_of(step), core_of(other)))

                @pl.when(other > 0)
                def _():
                    side[step, jnp.maximum(other - 1, 0)] = total.astype(bf16)
                    side_copy(step, jnp.maximum(other, 1)).start()

                @pl.when(jnp.logical_and(j == 0, step < n_samp - 1))
                def _():
                    chip[step + 1] = chip_total(step + 1).astype(bf16)
                    chip_copy(step + 1).start()

                @pl.when(other == 0)
                def _():
                    own[...] = total

            loop(0, n_rhs, by_core)

        loop(0, n_samp, leave)
        total = chip_total(0)
        for step in range(n_samp - 1, 0, -1):
            chip_copy(step).wait_recv()
            total = total + chip_in[step].astype(f32)
        applied[...] = total + RIDGE * direction[...]

        end_pieces(side_of)
        for step in range(1, n_samp):
            chip_copy(step).wait_send()
        for step in range(n_samp):
            for other in range(1, n_rhs):
                side_copy(step, other).wait_send()

        def end_chunk(c):
            up_copy(c).wait_send()

            @pl.when(has_prev)
            def _():
                down_copy(c).wait_send()

        loop(0, count, end_chunk)

        @pl.when(turn == ITERS - 1)
        def _():
            for step in range(1, n):
                rest_copy(step).wait_send()
                rest_copy(step).wait_recv()

    shrink = shrink_ref[...]
    factor_inner(right_ref[...].astype(bf16))
    f_first()
    residual[...] = right_ref[...]
    sol[...] = jnp.zeros_like(sol)
    f_second()
    f_third()
    f_fourth()
    projected[...] = factor_total()
    f_end()
    direction[...] = residual[...] + in_parts(shrink * projected[...], basis[...], 1)

    def iteration(turn):
        side_of = lax.rem(turn, 2)
        last = turn == ITERS - 1
        more = turn < ITERS - 1
        give_out(direction[...], side_of)
        operate(turn, side_of)
        block = dot_t(
            jnp.concatenate([direction[...], applied[...]], axis=0),
            jnp.concatenate([applied[...], residual[...]], axis=0),
        )
        for index in range(n):
            g_send[index] = block[index * g_rows : (index + 1) * g_rows]
        g_first()

        @pl.when(more)
        def _():
            factor_inner(applied[...].astype(bf16))
            f_first()

        @pl.when(last)
        def _():
            give_out(applied[...], 1 - side_of)

        g_second()

        @pl.when(more)
        def _():
            f_second()

        g_third()

        @pl.when(more)
        def _():
            f_third()

        @pl.when(last)
        def _():
            take_in(1 - side_of, None)

        g_fourth()
        summed = g_out[...].reshape(2 * width, 2 * width)
        g_end()
        gram = summed[:width, :width]
        inverse = inverse_of(0.5 * (gram + gram.T))
        back = dot_h(inverse, summed[:width, width:])
        back_t = back.T
        back_ref[...] = back_t
        mine = back_ref[pl.ds(pl.multiple_of(core * share, 8), share), :]
        sol[...] = sol[...] + in_parts(mine, narrow[side_of], 0)

        @pl.when(more)
        def _():
            left = residual[...] - dot_h(back_t, applied[...])
            residual[...] = left
            f_fourth()
            factor_image = factor_total()
            f_end()
            projection = projected[...] - dot_h(back_t, factor_image)
            projected[...] = projection
            scaled = left + in_parts(shrink * projection, basis[...], 1)
            image_new = summed[width:, width:] - dot_h(summed[width:, :width], back)
            image_new = image_new + dot_t(factor_image, shrink * projection)
            next_t = dot_h(inverse, image_new).T
            direction[...] = scaled - dot_h(next_t, direction[...])

        @pl.when(last)
        def _():
            acc[:share, :] = rest_in[...].astype(f32) - in_parts(mine, narrow[1 - side_of], 0)
            end_pieces(1 - side_of)

    loop(0, ITERS, iteration)
    first_out = pltpu.make_async_copy(sol, sol_out, out_sem.at[0])
    second_out = pltpu.make_async_copy(acc.at[pl.ds(0, share), :], res_out, out_sem.at[1])
    first_out.start()
    second_out.start()
    first_out.wait()
    second_out.wait()


def solve(n_samp, n_rhs, n_feat, right, basis, shrink, design):
    width, piece = right.shape
    rows, feats = design.shape
    rank = basis.shape[1]
    n = n_samp * n_rhs
    chunk = min(512, rows // 4)
    count = rows // chunk
    held = min(count, SLOT_BYTES // (chunk * feats * 2))
    share = width // n_rhs
    wide = (width, piece)
    blocks = (count, width, chunk)
    g_part = (2 * width // n, 2 * width)
    f_part = (width // n_samp, rank // n_rhs)
    vmem, dma = pltpu.VMEM, pltpu.SemaphoreType.DMA
    bf16, f32 = jnp.bfloat16, jnp.float32
    in_vmem, anywhere = pl.BlockSpec(memory_space=vmem), pl.BlockSpec(memory_space=pl.ANY)
    return pl.pallas_call(
        functools.partial(solve_kernel, n_samp, n_rhs, n_feat),
        name="solve",
        out_shape=[jax.ShapeDtypeStruct((share, feats), f32)] * 2,
        in_specs=[in_vmem, in_vmem, in_vmem, anywhere],
        out_specs=[anywhere, anywhere],
        scratch_shapes=[
            vmem((held, chunk, feats), bf16), vmem((2, width, feats), bf16),
            vmem((width, feats), f32),
            vmem(blocks, f32), vmem(blocks, bf16), vmem(blocks, bf16), vmem(blocks, bf16),
            vmem(blocks, bf16),
            vmem((n_samp, n_rhs - 1) + wide, bf16), vmem((n_samp, n_rhs - 1) + wide, bf16),
            vmem((n_samp,) + wide, bf16), vmem((n_samp,) + wide, bf16), vmem(wide, f32),
            vmem(wide, bf16), vmem(wide, f32), vmem(wide, f32), vmem(wide, f32),
            vmem((width, rank), f32), vmem((width, width), f32), vmem((share, feats), f32),
            vmem(wide, bf16), vmem((share, feats), bf16),
            vmem((n,) + g_part, f32), vmem((n,) + g_part, f32), vmem(g_part, f32),
            vmem((n_feat,) + g_part, f32), vmem((n,) + g_part, f32),
            vmem((n,) + f_part, bf16), vmem((n,) + f_part, bf16), vmem(f_part, bf16),
            vmem((n_feat,) + f_part, bf16), vmem((n,) + f_part, bf16),
            dma((held,)), dma((2,)), dma((n_samp,)), dma((n_samp,)),
            dma((n_samp, n_rhs)), dma((n_samp, n_rhs)),
            dma((count,)), dma((count,)), dma((count,)), dma((count,)), dma((count,)),
            dma((n_samp, n_rhs)), dma((n_samp, n_rhs)), dma((n_samp,)), dma((n_samp,)),
            dma((n,)), dma((n,)),
            dma((4, n)), dma((2, n_feat)), dma((4, n)), dma((2, n_feat)),
        ],
        compiler_params=pltpu.CompilerParams(
            collective_id=1, has_side_effects=True, vmem_limit_bytes=62 << 20
        ),
    )(right, basis, shrink, design)


def shards(n_samp, n_feat, n_rhs, design, right_side, factor, nystrom_values):
    feat_rows = right_side.shape[0]
    n = n_samp * n_rhs
    piece = feat_rows // n
    samp, rhs = lax.axis_index("samples"), lax.axis_index("rhs")
    shrink = (1.0 + jnp.min(nystrom_values)) / (1.0 + nystrom_values) - 1.0

    def own_rows(block):
        def rows_for(core):
            return lax.dynamic_slice_in_dim(block, (samp * n_rhs + core) * piece, piece, 0)

        parts = [None] * n_rhs
        moved = [rows_for(rhs)]
        for step in range(1, n_rhs):
            pairs = [(i, (i + step) % n_rhs) for i in range(n_rhs)]
            moved.append(lax.ppermute(rows_for((rhs + step) % n_rhs), "rhs", pairs))
        for core in range(n_rhs):
            best = moved[0]
            for step in range(1, n_rhs):
                best = jnp.where((rhs - step) % n_rhs == core, moved[step], best)
            parts[core] = best
        return jnp.concatenate(parts, axis=1)

    basis = own_rows(factor)
    residual = own_rows(right_side).T
    sol, res = solve(n_samp, n_rhs, n_feat, residual, basis, shrink[None, :], design)
    return sol.T, res.T


def solution(mesh):
    placed = (P(("samples", "rhs"), "features"), P("features", "rhs"), P("features", "rhs"), P())
    sizes = (mesh.shape["samples"], mesh.shape["features"], mesh.shape["rhs"])
    return jax.shard_map(
        functools.partial(shards, *sizes),
        mesh=mesh,
        in_specs=placed,
        out_specs=(P("features", "rhs"), P("features", "rhs")),
        check_vma=False,
    )
```

```python
import functools

import jax
import jax.numpy as jnp
from jax import lax
from jax.experimental import pallas as pl
from jax.experimental.pallas import tpu as pltpu
from jax.sharding import PartitionSpec as P

ITERS = 3
MESH = pl.DeviceIdType.MESH
RIDGE = 1.0
EARLY = 3
LATE = 2
SLOT_BYTES = 40 << 20


def dot_t(left, right):
    return lax.dot_general(
        left,
        right,
        (((1,), (1,)), ((), ())),
        precision=lax.Precision.HIGHEST,
        preferred_element_type=jnp.float32,
    )


def dot_h(left, right):
    return jnp.dot(
        left, right, precision=lax.Precision.HIGHEST, preferred_element_type=jnp.float32
    )


def columns(index, width):
    return pl.ds(pl.multiple_of(index * width, 128), width)


def partner(me, step, n):
    bit, total = 1, 0
    while bit < n:
        total = total + (me // bit + step // bit) % 2 * bit
        bit *= 2
    return total


def loop(start, stop, body):
    def step(i, carry):
        body(i)
        return carry

    lax.fori_loop(start, stop, step, 0)


def parts_of(values):
    upper = values.astype(jnp.bfloat16)
    lower = (values - upper.astype(jnp.float32)).astype(jnp.bfloat16)
    return jnp.concatenate([upper, lower], axis=0)


def in_parts(values, right, contract):
    rows = values.shape[0]
    both = lax.dot_general(
        parts_of(values), right, (((1,), (contract,)), ((), ())),
        preferred_element_type=jnp.float32,
    )
    return both[:rows] + both[rows:]


def inverse_of(gram):
    size = gram.shape[0]
    rows = lax.broadcasted_iota(jnp.int32, (size, 2 * size), 0)
    lanes = lax.broadcasted_iota(jnp.int32, (size, 2 * size), 1)
    unit = (lanes == rows + size).astype(jnp.float32)
    work = jnp.concatenate([gram, jnp.zeros_like(gram)], axis=1) + unit
    for k in range(size):
        pivot = work[k : k + 1, :] / work[k : k + 1, k : k + 1]
        work = jnp.where(rows == k, pivot, work - work[:, k : k + 1] * pivot)
    return work[:, size:]


def solve_kernel(
    n_samp, n_rhs, n_feat,
    right_ref, factor, values_ref, design, sol_out, res_out,
    basis, slots, narrow, acc, part, up, cross, images, give, side, side_in, chip, chip_in,
    sent, direction, applied, residual, projected, back_ref, sol, rest, rest_in,
    g_send, g_held, g_mine, g_across, g_out, f_send, f_held, f_mine, f_across, f_out,
    load_sem, out_sem, piece_send, piece_recv, twin_send, twin_recv,
    up_send, up_recv, cross_recv, down_send, down_recv,
    side_send, side_recv, chip_send, chip_recv, rest_send, rest_recv,
    g_sems, gz_sems, f_sems, fz_sems, basis_sems,
):
    samp, core = lax.axis_index("samples"), lax.axis_index("rhs")
    feat = lax.axis_index("features")
    n = n_samp * n_rhs
    me = samp * n_rhs + core
    count, width, chunk = images.shape
    ring = part.shape[0]
    held = slots.shape[0]
    spare = count - held
    piece = residual.shape[1]
    share = width // n_rhs
    half = n_feat // 2
    low = feat < half
    inner = jnp.logical_or(feat == half - 1, feat == half)
    outer = jnp.logical_not(inner)
    is_end = jnp.logical_or(feat == 0, feat == n_feat - 1)
    has_prev = jnp.logical_not(is_end)
    following = jnp.where(low, feat + 1, feat - 1)
    before = jnp.where(low, feat - 1, feat + 1)
    f32, bf16 = jnp.float32, jnp.bfloat16

    def place(index):
        return {"samples": lax.div(index, n_rhs), "rhs": lax.rem(index, n_rhs)}

    def chip_of(step):
        return partner(samp, step, n_samp)

    def core_of(step):
        return partner(core, step, n_rhs)

    def cols(chip_index, core_index):
        return columns(chip_index * n_rhs + core_index, piece)

    def remote(src, dst, send, recv, where):
        return pltpu.make_async_remote_copy(
            src_ref=src, dst_ref=dst, send_sem=send, recv_sem=recv,
            device_id=where, device_id_type=MESH,
        )

    def slot_of(turn, c):
        return lax.rem(turn * spare + c, held)

    def load(turn, c, slot):
        later = spare + lax.rem(c - spare + held + spare * turn, held)
        row = pl.multiple_of(jnp.where(c < spare, c, later) * chunk, chunk)
        return pltpu.make_async_copy(
            design.at[pl.ds(row, chunk), :], slots.at[slot], load_sem.at[slot]
        )

    def load_first(turn, c):
        return load(turn, c, slot_of(turn, c))

    def load_again(turn, c):
        return load(turn, c, slot_of(turn, c + spare))

    right_copy = pltpu.make_async_copy(right_ref, residual, out_sem.at[0])
    right_copy.start()

    barrier = pltpu.get_barrier_semaphore()
    for step in range(1, n):
        pl.semaphore_signal(
            barrier, inc=1, device_id=place(lax.rem(me + step, n)), device_id_type=MESH
        )
    for step in range(1, n_feat):
        pl.semaphore_signal(
            barrier, inc=1, device_id={"features": lax.rem(feat + step, n_feat)},
            device_id_type=MESH,
        )
    pl.semaphore_wait(barrier, n - 1 + n_feat - 1)

    lanes = factor.shape[1]

    def factor_rows(core_index):
        return factor.at[pl.ds(pl.multiple_of((samp * n_rhs + core_index) * piece, 16), piece), :]

    factor_own = pltpu.make_async_copy(
        factor_rows(core), basis.at[:, columns(core, lanes)], basis_sems.at[0, 0]
    )

    def factor_copy(other):
        return remote(
            factor_rows(core_of(other)), basis.at[:, columns(core, lanes)],
            basis_sems.at[0, other], basis_sems.at[1, other], {"rhs": core_of(other)},
        )

    for other in range(1, n_rhs):
        factor_copy(other).start()
    factor_own.start()
    loop(0, held, lambda c: load_first(0, c).start())

    def totals(send, held_in, mine, across, out, sems, z_sems):
        def scatter(step):
            peer = lax.rem(me + step, n)
            return remote(
                send.at[peer], held_in.at[me], sems.at[0, step], sems.at[1, step], place(peer)
            )

        def along(step):
            peer = lax.rem(feat + step, n_feat)
            return remote(
                mine, across.at[feat], z_sems.at[0, step], z_sems.at[1, step], {"features": peer}
            )

        def gather(step):
            peer = lax.rem(me + step, n)
            return remote(
                out.at[me], out.at[me], sems.at[2, step], sems.at[3, step], place(peer)
            )

        def first():
            for step in range(1, n):
                scatter(step).start()

        def second():
            total = send[me].astype(f32)
            for step in range(1, n):
                scatter(step).wait_recv()
            for step in range(1, n):
                total = total + held_in[lax.rem(me + step, n)].astype(f32)
            mine[...] = total.astype(mine.dtype)
            for step in range(1, n_feat):
                along(step).start()
            across[feat] = total.astype(mine.dtype)

        def third():
            for step in range(1, n_feat):
                along(step).wait_recv()
            total = across[0].astype(f32)
            for index in range(1, n_feat):
                total = total + across[index].astype(f32)
            out[me] = total.astype(out.dtype)
            for step in range(1, n):
                gather(step).start()

        def fourth():
            for step in range(1, n):
                gather(step).wait_recv()

        def end():
            for step in range(1, n):
                scatter(step).wait_send()
                gather(step).wait_send()
            for step in range(1, n_feat):
                along(step).wait_send()

        return first, second, third, fourth, end

    g_first, g_second, g_third, g_fourth, g_end = totals(
        g_send, g_held, g_mine, g_across, g_out, g_sems, gz_sems
    )
    f_first, f_second, f_third, f_fourth, f_end = totals(
        f_send, f_held, f_mine, f_across, f_out, f_sems, fz_sems
    )
    f_rows, f_lanes = f_send.shape[1:]
    g_rows = g_send.shape[1]

    def factor_inner(values):
        inner_product = jnp.dot(values, basis[...], preferred_element_type=f32)
        for s in range(n_samp):
            for c in range(n_rhs):
                block = inner_product[s * f_rows : (s + 1) * f_rows, c * f_lanes : (c + 1) * f_lanes]
                f_send[s * n_rhs + c] = block.astype(bf16)

    def factor_total():
        lines = []
        for s in range(n_samp):
            line = [f_out[s * n_rhs + c].astype(f32) for c in range(n_rhs)]
            lines.append(jnp.concatenate(line, axis=1))
        return jnp.concatenate(lines, axis=0)

    def piece_copy(step, side_of):
        return remote(
            sent, narrow.at[side_of, :, cols(samp, core)], piece_send.at[step],
            piece_recv.at[step], {"samples": chip_of(step)},
        )

    def twin_copy(step, other, side_of):
        block = narrow.at[side_of, :, cols(chip_of(step), core)]
        return remote(
            block, block, twin_send.at[step, other], twin_recv.at[step, other],
            {"rhs": core_of(other)},
        )

    def give_out(values, side_of):
        sent[...] = values.astype(bf16)
        for step in range(1, n_samp):
            piece_copy(step, side_of).start()
        narrow[side_of, :, cols(samp, core)] = values.astype(bf16)

    def take_in(side_of, use):
        def arrive(step):
            @pl.when(step > 0)
            def _():
                piece_copy(step, side_of).wait_recv()

            for other in range(1, n_rhs):
                twin_copy(step, other, side_of).start()

            def by_core(other):
                @pl.when(other > 0)
                def _():
                    twin_copy(step, other, side_of).wait_recv()

                if use is not None:
                    use(cols(chip_of(step), core_of(other)))

            loop(0, n_rhs, by_core)

        loop(0, n_samp, arrive)

    def end_pieces(side_of):
        for step in range(1, n_samp):
            piece_copy(step, side_of).wait_send()
        for step in range(n_samp):
            for other in range(1, n_rhs):
                twin_copy(step, other, side_of).wait_send()

    def up_copy(c):
        return remote(
            give.at[c], up.at[c], up_send.at[c], up_recv.at[c], {"features": following}
        )

    def cross_copy(c):
        return remote(
            give.at[c], cross.at[c], up_send.at[c], cross_recv.at[c], {"features": following}
        )

    def down_copy(c):
        return remote(
            images.at[c], images.at[c], down_send.at[c], down_recv.at[c], {"features": before}
        )

    def pass_up(c):
        @pl.when(inner)
        def _():
            cross_copy(c).start()

        @pl.when(outer)
        def _():
            up_copy(c).start()

    def up_first(c):
        @pl.when(is_end)
        def _():
            give[c] = part[lax.rem(c, ring)].astype(bf16)
            pass_up(c)

    def up_step(c):
        @pl.when(has_prev)
        def _():
            up_copy(c).wait_recv()
            total = part[lax.rem(c, ring)] + up[c].astype(f32)
            part[lax.rem(c, ring)] = total
            give[c] = total.astype(bf16)
            pass_up(c)

    def cross_step(c):
        @pl.when(inner)
        def _():
            cross_copy(c).wait_recv()
            images[c] = (part[lax.rem(c, ring)] + cross[c].astype(f32)).astype(bf16)

            @pl.when(has_prev)
            def _():
                down_copy(c).start()

    def ready(c):
        @pl.when(outer)
        def _():
            down_copy(c).wait_recv()

            @pl.when(has_prev)
            def _():
                down_copy(c).start()

    def side_copy(step, other):
        return remote(
            side.at[step, other - 1], side_in.at[step, other - 1],
            side_send.at[step, other], side_recv.at[step, other], {"rhs": core_of(other)},
        )

    def chip_copy(step):
        return remote(
            chip.at[step - 1], chip_in.at[step - 1], chip_send.at[step], chip_recv.at[step],
            {"samples": chip_of(step)},
        )

    def chip_total(step):
        total = applied[...]
        for other in range(1, n_rhs):
            side_copy(step, other).wait_recv()
            total = total + side_in[step, other - 1].astype(f32)
        return total

    def operate(turn, side_of):
        acc[...] = jnp.zeros_like(acc)
        for c in range(EARLY):
            part[lax.rem(c, ring)] = jnp.zeros((width, chunk), f32)

        @pl.when(turn == 0)
        def _():
            for c in range(EARLY):
                load_first(turn, c).wait()

        def first_terms(place_cols):
            for c in range(EARLY):
                part[lax.rem(c, ring)] = part[lax.rem(c, ring)] + lax.dot_general(
                    narrow[side_of, :, place_cols], slots[slot_of(turn, c), :, place_cols],
                    (((1,), (1,)), ((), ())), preferred_element_type=f32,
                )

        take_in(side_of, first_terms)

        def rest_copy(step):
            peer = lax.rem(me + step, n)
            row = pl.multiple_of(lax.rem(peer, n_rhs) * share, 16)
            return remote(
                rest.at[pl.ds(row, share), :], rest_in.at[:, columns(me, piece)],
                rest_send.at[step], rest_recv.at[step], place(peer),
            )

        @pl.when(turn == ITERS - 1)
        def _():
            rest[...] = residual[...].astype(bf16)
            for step in range(1, n):
                rest_copy(step).start()
            rest_in[:, columns(me, piece)] = rest[pl.ds(pl.multiple_of(core * share, 16), share), :]

        for c in range(EARLY):
            up_first(c)
            if c < spare:
                load_first(turn, c + held).start()

        def summed_by(c):
            return jnp.where(c > EARLY, c, jnp.where(c == EARLY, 1, 0))

        def image_step(c):
            @pl.when(jnp.logical_or(turn == 0, c >= held))
            def _():
                load_first(turn, c).wait()

            part[lax.rem(c, ring)] = lax.dot_general(
                narrow[side_of], slots[slot_of(turn, c)],
                (((1,), (1,)), ((), ())), preferred_element_type=f32,
            )
            up_first(c)

            @pl.when(c < spare)
            def _():
                load_first(turn, c + held).start()

            loop(summed_by(c - 1), summed_by(c), up_step)
            loop(summed_by(c - 2), summed_by(c - 1), cross_step)

        loop(EARLY, count, image_step)
        kept = count - LATE - spare

        def feature_step(i):
            c = jnp.where(i < kept, spare + i, i - kept)
            again = c < spare

            @pl.when(again)
            def _():
                load_again(turn, c).wait()

            ready(c)
            acc[...] = acc[...] + jnp.dot(
                images[c], slots[slot_of(turn, jnp.where(again, c + spare, c))],
                preferred_element_type=f32,
            )

            @pl.when(i < spare)
            def _():
                load_again(turn, i).start()

            @pl.when(i == 1)
            def _():
                up_step(count - 1)
                cross_step(count - 2)

            @pl.when(i == 3)
            def _():
                cross_step(count - 1)

        loop(0, count - LATE, feature_step)
        for c in range(count - LATE, count):
            ready(c)

        def piece_total(place_cols):
            total = acc[:, place_cols]
            for c in range(count - LATE, count):
                total = total + jnp.dot(
                    images[c], slots[slot_of(turn, c), :, place_cols], preferred_element_type=f32
                )
            return total

        def leave(i):
            step = n_samp - 1 - i

            def by_core(j):
                other = n_rhs - 1 - j
                total = piece_total(cols(chip_of(step), core_of(other)))

                @pl.when(other > 0)
                def _():
                    side[step, jnp.maximum(other - 1, 0)] = total.astype(bf16)
                    side_copy(step, jnp.maximum(other, 1)).start()

                @pl.when(jnp.logical_and(j == 0, step < n_samp - 1))
                def _():
                    chip[step] = chip_total(step + 1).astype(bf16)
                    chip_copy(step + 1).start()

                @pl.when(other == 0)
                def _():
                    applied[...] = total

            loop(0, n_rhs, by_core)

        loop(0, n_samp, leave)
        total = chip_total(0)
        for step in range(n_samp - 1, 0, -1):
            chip_copy(step).wait_recv()
            total = total + chip_in[step - 1].astype(f32)
        applied[...] = total + RIDGE * direction[...]

        end_pieces(side_of)
        for step in range(1, n_samp):
            chip_copy(step).wait_send()
        for step in range(n_samp):
            for other in range(1, n_rhs):
                side_copy(step, other).wait_send()

        def end_chunk(c):
            up_copy(c).wait_send()

            @pl.when(has_prev)
            def _():
                down_copy(c).wait_send()

        loop(0, count, end_chunk)

        @pl.when(turn == ITERS - 1)
        def _():
            for step in range(1, n):
                rest_copy(step).wait_send()
                rest_copy(step).wait_recv()

    values = values_ref[...]
    shrink = (1.0 + jnp.min(values, axis=1, keepdims=True)) / (1.0 + values) - 1.0
    right_copy.wait()
    factor_own.wait()
    for other in range(1, n_rhs):
        factor_copy(other).wait()
    factor_inner(residual[...].astype(bf16))
    f_first()
    sol[...] = jnp.zeros_like(sol)
    f_second()
    f_third()
    f_fourth()
    projected[...] = factor_total()
    f_end()
    direction[...] = residual[...] + in_parts(shrink * projected[...], basis[...], 1)

    def iteration(turn):
        side_of = lax.rem(turn, 2)
        last = turn == ITERS - 1
        more = turn < ITERS - 1
        give_out(direction[...], side_of)
        operate(turn, side_of)
        block = dot_t(
            jnp.concatenate([direction[...], applied[...]], axis=0),
            jnp.concatenate([applied[...], residual[...]], axis=0),
        )
        for index in range(n):
            g_send[index] = block[index * g_rows : (index + 1) * g_rows]
        g_first()

        @pl.when(more)
        def _():
            factor_inner(applied[...].astype(bf16))
            f_first()

        @pl.when(last)
        def _():
            give_out(applied[...], 1 - side_of)

        g_second()

        @pl.when(more)
        def _():
            f_second()

        g_third()

        @pl.when(more)
        def _():
            f_third()

        @pl.when(last)
        def _():
            take_in(1 - side_of, None)

        g_fourth()
        summed = g_out[...].reshape(2 * width, 2 * width)
        g_end()
        gram = summed[:width, :width]
        inverse = inverse_of(0.5 * (gram + gram.T))
        back = dot_h(inverse, summed[:width, width:])
        back_t = back.T
        back_ref[...] = back_t
        mine = back_ref[pl.ds(pl.multiple_of(core * share, 8), share), :]
        sol[...] = sol[...] + in_parts(mine, narrow[side_of], 0)

        @pl.when(more)
        def _():
            left = residual[...] - dot_h(back_t, applied[...])
            residual[...] = left
            f_fourth()
            factor_image = factor_total()
            f_end()
            projection = projected[...] - dot_h(back_t, factor_image)
            projected[...] = projection
            scaled = left + in_parts(shrink * projection, basis[...], 1)
            image_new = summed[width:, width:] - dot_h(summed[width:, :width], back)
            image_new = image_new + dot_t(factor_image, shrink * projection)
            next_t = dot_h(inverse, image_new).T
            direction[...] = scaled - dot_h(next_t, direction[...])

        @pl.when(last)
        def _():
            acc[:share, :] = rest_in[...].astype(f32) - in_parts(mine, narrow[1 - side_of], 0)
            end_pieces(1 - side_of)

    loop(0, ITERS, iteration)
    first_out = pltpu.make_async_copy(sol, sol_out, out_sem.at[0])
    second_out = pltpu.make_async_copy(acc.at[pl.ds(0, share), :], res_out, out_sem.at[1])
    first_out.start()
    second_out.start()
    first_out.wait()
    second_out.wait()


def solve(n_samp, n_rhs, n_feat, right, factor, values, design):
    width, piece = right.shape
    rows, feats = design.shape
    rank = values.shape[1]
    n = n_samp * n_rhs
    chunk = min(512, rows // 4)
    count = rows // chunk
    held = min(count, SLOT_BYTES // (chunk * feats * 2))
    share = width // n_rhs
    wide = (width, piece)
    blocks = (count, width, chunk)
    g_part = (2 * width // n, 2 * width)
    f_part = (width // n_samp, rank // n_rhs)
    vmem, dma = pltpu.VMEM, pltpu.SemaphoreType.DMA
    bf16, f32 = jnp.bfloat16, jnp.float32
    in_vmem, anywhere = pl.BlockSpec(memory_space=vmem), pl.BlockSpec(memory_space=pl.ANY)
    return pl.pallas_call(
        functools.partial(solve_kernel, n_samp, n_rhs, n_feat),
        name="solve",
        out_shape=[jax.ShapeDtypeStruct((share, feats), f32)] * 2,
        in_specs=[anywhere, anywhere, in_vmem, anywhere],
        out_specs=[anywhere, anywhere],
        scratch_shapes=[
            vmem((piece, rank), bf16),
            vmem((held, chunk, feats), bf16), vmem((2, width, feats), bf16),
            vmem((width, feats), f32),
            vmem((min(count, 6), width, chunk), f32), vmem(blocks, bf16), vmem(blocks, bf16), vmem(blocks, bf16),
            vmem(blocks, bf16),
            vmem((n_samp, n_rhs - 1) + wide, bf16), vmem((n_samp, n_rhs - 1) + wide, bf16),
            vmem((n_samp - 1,) + wide, bf16), vmem((n_samp - 1,) + wide, bf16),
            vmem(wide, bf16), vmem(wide, f32), vmem(wide, f32), vmem(wide, f32),
            vmem((width, rank), f32), vmem((width, width), f32), vmem((share, feats), f32),
            vmem(wide, bf16), vmem((share, feats), bf16),
            vmem((n,) + g_part, f32), vmem((n,) + g_part, f32), vmem(g_part, f32),
            vmem((n_feat,) + g_part, f32), vmem((n,) + g_part, f32),
            vmem((n,) + f_part, bf16), vmem((n,) + f_part, bf16), vmem(f_part, bf16),
            vmem((n_feat,) + f_part, bf16), vmem((n,) + f_part, bf16),
            dma((held,)), dma((2,)), dma((n_samp,)), dma((n_samp,)),
            dma((n_samp, n_rhs)), dma((n_samp, n_rhs)),
            dma((count,)), dma((count,)), dma((count,)), dma((count,)), dma((count,)),
            dma((n_samp, n_rhs)), dma((n_samp, n_rhs)), dma((n_samp,)), dma((n_samp,)),
            dma((n,)), dma((n,)),
            dma((4, n)), dma((2, n_feat)), dma((4, n)), dma((2, n_feat)), dma((2, n_rhs)),
        ],
        compiler_params=pltpu.CompilerParams(
            collective_id=1, has_side_effects=True, vmem_limit_bytes=62 << 20
        ),
    )(right, factor, values, design)


def shards(n_samp, n_feat, n_rhs, design, right_side, factor, nystrom_values):
    feat_rows = right_side.shape[0]
    n = n_samp * n_rhs
    piece = feat_rows // n
    samp, rhs = lax.axis_index("samples"), lax.axis_index("rhs")

    def own_rows(block):
        def rows_for(core):
            return lax.dynamic_slice_in_dim(block, (samp * n_rhs + core) * piece, piece, 0)

        parts = [None] * n_rhs
        moved = [rows_for(rhs)]
        for step in range(1, n_rhs):
            pairs = [(i, (i + step) % n_rhs) for i in range(n_rhs)]
            moved.append(lax.ppermute(rows_for((rhs + step) % n_rhs), "rhs", pairs))
        for core in range(n_rhs):
            best = moved[0]
            for step in range(1, n_rhs):
                best = jnp.where((rhs - step) % n_rhs == core, moved[step], best)
            parts[core] = best
        return jnp.concatenate(parts, axis=1)

    residual = own_rows(right_side).T
    sol, res = solve(n_samp, n_rhs, n_feat, residual, factor, nystrom_values[None, :], design)
    return sol.T, res.T


def solution(mesh):
    placed = (P(("samples", "rhs"), "features"), P("features", "rhs"), P("features", "rhs"), P())
    sizes = (mesh.shape["samples"], mesh.shape["features"], mesh.shape["rhs"])
    return jax.shard_map(
        functools.partial(shards, *sizes),
        mesh=mesh,
        in_specs=placed,
        out_specs=(P("features", "rhs"), P("features", "rhs")),
        check_vma=False,
    )
```
